32 devices in a mesh: leaf: 8 (over z, y), probe: 4 (over x, core).
Axes of the slice: x: 2, y: 2, z: 4, core: 2. Of those that a mesh axis runs over, the one named last changes fastest.
Arguments:
- coords: float32 [3, 32768], P(None, 'leaf')
- site_order: int32 [128, 256], P('leaf'), may hold values from 0 to 255, each once within a row
- leaf_pairs: int32 [2, 768], P(None, 'leaf'), may hold values from 0 to 127, as said below
- pair_count: int32 [8], P('leaf'), may hold values from 31 to 96, as said below
- probes: float32 [64, 32768], P('probe', 'leaf'), may hold values from -16 to 16
Outputs:
- solution: float32 [64, 32768], P('probe', 'leaf')
- residual: float32 [64, 32768], P('probe', 'leaf')
The draws below stay inside these ranges and needn't reach their ends.
Inputs may be any that keep to these rules, and one draw needn't show every extreme that they name: `leaf_pairs`: each leaf index owns 96 slots; its first pair_count slots hold distinct pairs (i, j) with i among that index's own 16 leaves and i <= j <= i + 5, j < 128, every own leaf listed with itself once and with the next leaf where there is one; the later slots hold the index's first leaf twice. `pair_count`: pairs listed for each leaf index; some index lists 96 in every draw. Each row of site_order lists 0 to 255 once.
All inputs are finite; a program needn't handle non-finite values.
Results may differ from the reference program's by a relative error of at most 0.0003.
Values sent between devices are 32-bit elements; how exact they have to be, the bound alone decides.
A program may use at most 64 MiB of HBM per device.

```python
import math
import jax
import jax.numpy as jnp
from jax import lax

LEAF = 256
REACH = 5
PROBES = 64
ITERS = 2
LEAF_DEV = 16
LEAVES = 128
SITES = 32768


UNIT = 0.025


SIDE = 0.5


def slab_layout(key):
    groups = LEAVES // LEAF_DEV
    k_wide, k_dense, k_force = jax.random.split(jax.random.fold_in(key, 7), 3)
    widths = jax.random.randint(k_wide, (LEAVES,), 2, REACH + 1)
    flagged = jax.random.randint(k_dense, (groups,), 0, 8) == 0
    forced = jax.random.randint(k_force, (), 0, groups - 1)
    leaf_ids = jnp.arange(LEAVES)
    owner = leaf_ids // LEAF_DEV
    follow = (leaf_ids >= (forced + 1) * LEAF_DEV) & (leaf_ids < (forced + 1) * LEAF_DEV + REACH - 1)
    crowded = flagged[owner] | (owner == forced) | follow
    widths = jnp.where(crowded, 1, widths)
    ends = jnp.cumsum(widths)
    start_offsets = ends - widths
    return (widths, start_offsets, ends)


def pair_table(key):
    widths, start_offsets, ends = slab_layout(key)
    groups = LEAVES // LEAF_DEV
    slots = LEAF_DEV * (REACH + 1)
    leaf_ids = jnp.arange(LEAVES)
    offsets = jnp.arange(REACH + 1)
    partner = leaf_ids[:, None] + offsets[None, :]
    inside = partner < LEAVES
    capped = jnp.minimum(partner, LEAVES - 1)
    near = start_offsets[capped] - ends[:, None] < REACH
    valid = (inside & ((offsets[None, :] == 0) | near)).reshape(groups, slots)
    rows = jnp.broadcast_to(leaf_ids[:, None], partner.shape).reshape(groups, slots)
    cols = capped.reshape(groups, slots)
    sorted_rank = jnp.argsort(1 - valid.astype(jnp.int32), axis=1, stable=True)
    rows = jnp.take_along_axis(rows, sorted_rank, axis=1)
    cols = jnp.take_along_axis(cols, sorted_rank, axis=1)
    count = jnp.sum(valid.astype(jnp.int32), axis=1)
    live = jnp.arange(slots)[None, :] < count[:, None]
    first = (jnp.arange(groups) * LEAF_DEV)[:, None]
    rows = jnp.where(live, rows, first)
    cols = jnp.where(live, cols, first)
    return (jnp.stack([rows.reshape(-1), cols.reshape(-1)]).astype(jnp.int32), count.astype(jnp.int32))


def draw_leaf_pairs(key, part):
    return pair_table(key)[0]


def draw_pair_count(key, part):
    return pair_table(key)[1]


def draw_coords(key, part):
    widths, start_offsets, ends = slab_layout(key)
    k_along, k_across = jax.random.split(jax.random.fold_in(key, 11))
    along = jax.random.uniform(k_along, (LEAVES, LEAF), jnp.float32)
    first = (start_offsets[:, None].astype(jnp.float32) + widths[:, None].astype(jnp.float32) * along) * UNIT
    across = jax.random.uniform(k_across, (2, LEAVES, LEAF), jnp.float32) * SIDE
    return jnp.concatenate([first[None], across], axis=0).reshape(3, SITES).astype(jnp.float32)


def draw_probes(key, part):
    k_base, k_row, k_leaf = jax.random.split(jax.random.fold_in(key, 13), 3)
    base = jnp.clip(jax.random.normal(k_base, (PROBES, LEAVES, LEAF), jnp.float32), -4.0, 4.0)
    row_scale = jnp.exp(jax.random.uniform(k_row, (PROBES, 1, 1), jnp.float32, -1.15, 1.15))
    leaf_scale = jnp.exp(jax.random.uniform(k_leaf, (1, LEAVES, 1), jnp.float32, -1.15, 1.15))
    rising = jnp.exp(0.55 * jnp.arange(LEAVES, dtype=jnp.float32) / LEAVES)[None, :, None]
    values = jnp.clip(base * row_scale * leaf_scale * rising, -16.0, 16.0)
    return values.reshape(PROBES, SITES).astype(jnp.float32)


def setup_inputs(seed: int = 0) -> dict:
    streams_of = jax.random.split(jax.random.key(seed), 6)
    return {
        "coords": draw_coords(jax.random.fold_in(streams_of[5], 71), 0),
        "site_order": jax.vmap(lambda own: jax.random.permutation(own, LEAF))(jax.random.split(streams_of[1], LEAVES)).reshape((LEAVES, LEAF)).astype(jnp.int32),
        "leaf_pairs": draw_leaf_pairs(jax.random.fold_in(streams_of[5], 71), 0),
        "pair_count": draw_pair_count(jax.random.fold_in(streams_of[5], 71), 0),
        "probes": draw_probes(jax.random.fold_in(streams_of[5], 71), 0),
    }


UNIT = 0.025
LENGTH = 0.12
NUGGET = 0.5
UPPER_LIMIT = lax.Precision.HIGHEST

def kernel_tiles(left, right):
    diff = left[:, :, :, None] - right[:, :, None, :]
    dist = jnp.sqrt(lax.optimization_barrier(jnp.sum(diff * diff, axis=0)))
    taper = REACH * UNIT
    scaled = dist * (math.sqrt(3.0) / LENGTH)
    remain = jnp.maximum(1.0 - dist / taper, 0.0)
    return (1.0 + scaled) * jnp.exp(-scaled) * remain ** 4 * (1.0 + 4.0 * dist / taper)

def apply_operator(points, leaf_pairs, pair_count, field):
    groups = pair_count.shape[0]
    slots = leaf_pairs.shape[1] // groups

    def one_group(group, grand_total):

        def one_pair(index, acc):
            slot = group * slots + index
            row = leaf_pairs[0, slot]
            col = leaf_pairs[1, slot]
            tile = kernel_tiles(points[:, row][:, None], points[:, col][:, None])[0]
            to_row = jnp.dot(field[:, col], tile.T, precision=UPPER_LIMIT)
            column_target = jnp.dot(field[:, row], tile, precision=UPPER_LIMIT)
            column_target = jnp.where(row != col, column_target, jnp.zeros_like(column_target))
            acc = acc.at[:, row].add(to_row)
            return acc.at[:, col].add(column_target)
        return lax.fori_loop(0, pair_count[group], one_pair, grand_total)
    summed = lax.fori_loop(0, groups, one_group, jnp.zeros_like(field))
    return NUGGET * field + summed

def reference(coords, site_order, leaf_pairs, pair_count, probes):
    points = jnp.take_along_axis(coords.reshape(3, LEAVES, LEAF), site_order[None], axis=2)
    right = probes.reshape(PROBES, LEAVES, LEAF)
    solution = jnp.zeros_like(right)
    residual = right
    direction = right
    norm_now = lax.optimization_barrier(jnp.sum(residual * residual, axis=(1, 2)))
    for step in range(ITERS):
        image = apply_operator(points, leaf_pairs, pair_count, direction)
        alpha = norm_now / lax.optimization_barrier(jnp.sum(direction * image, axis=(1, 2)))
        solution = solution + alpha[:, None, None] * direction
        residual = residual - alpha[:, None, None] * image
        if step + 1 < ITERS:
            norm_next = lax.optimization_barrier(jnp.sum(residual * residual, axis=(1, 2)))
            direction = residual + (norm_next / norm_now)[:, None, None] * direction
            norm_now = norm_next
    return (solution.reshape(PROBES, SITES), residual.reshape(PROBES, SITES))
```

```python
import functools
import math

import jax
import jax.numpy as jnp
from jax import lax
from jax.experimental import pallas as pl
from jax.experimental.pallas import tpu as pltpu
from jax.sharding import PartitionSpec as P

REACH = 5
UNIT = 0.025
LENGTH = 0.12
NUGGET = 0.5
TAPER = REACH * UNIT
GROW = math.sqrt(3.0) * TAPER / LENGTH
QUAD = 4.0 * GROW
LIN = (4.0 + GROW) / QUAD
RATE = -GROW / math.log(2.0)
OFFS = REACH + 1
ROWS = 32
MESH = pl.DeviceIdType.MESH
F32 = jnp.float32
BF16 = jnp.bfloat16


def split(x):
    hi = x.astype(BF16)
    return hi, (x - hi.astype(F32)).astype(BF16)


def stacked(x):
    hi = x.astype(BF16).astype(F32)
    return jnp.concatenate([hi, x - hi], axis=0).astype(BF16)


def dot(a, b, ca, cb):
    return lax.dot_general(a, b, (((ca,), (cb,)), ((), ())), preferred_element_type=F32)


def fold(x):
    half = x.shape[0] // 2
    return x[:half] + x[half:]


def kernel(
    n, coords_ref, order_ref, pairs_ref, count_ref, probes_ref, sol_ref, res_ref,
    c8, prow, pcb, mask, tiles, v, v2, acc, r1, acc2, halo0, back0, back1, halo1,
    sum_out, sum_in, ssem, rsem, hsend, hrecv,
):
    leaf_dev, width = order_ref.shape
    cols = probes_ref.shape[0]
    extent = leaf_dev + REACH
    me = lax.axis_index("leaf")
    after = lax.rem(me + 1, n)
    before = lax.rem(me + n - 1, n)

    barrier = pltpu.get_barrier_semaphore()
    for k in range(1, n):
        pl.semaphore_signal(
            barrier, inc=1, device_id={"leaf": lax.rem(me + k, n)}, device_id_type=MESH
        )

    c8[...] = jnp.zeros_like(c8)
    c8[0:3, :] = coords_ref[...] * (1.0 / TAPER)
    place = lax.broadcasted_iota(jnp.int32, (width, width), 0)

    for l in range(leaf_dev):
        x = c8[:, l * width : (l + 1) * width]
        hi = x.astype(BF16).astype(F32)
        mid = (x - hi).astype(BF16).astype(F32)
        parts = jnp.concatenate([hi, mid, x - hi - mid], axis=0).astype(BF16)
        onehot = jnp.where(place == order_ref[l : l + 1, :], 1.0, 0.0).astype(BF16)
        got = dot(parts, onehot, 1, 0)
        prow[l] = got[0:8] + got[8:16] + got[16:24]

    slots = pairs_ref.shape[1]
    first = pairs_ref[0:1, :]
    second = pairs_ref[1:2, :]
    code = (first - me * leaf_dev) * OFFS + (second - first)
    lane = lax.broadcasted_iota(jnp.int32, (1, slots), 1)
    code = jnp.where(lane < count_ref[0], code, -1)
    want = lax.broadcasted_iota(jnp.int32, (leaf_dev * OFFS, slots), 0)
    hit = jnp.max(jnp.where(want == code, 1.0, 0.0), axis=1, keepdims=True)
    mask[...] = jnp.broadcast_to(hit, mask.shape)

    rr = jnp.zeros((cols, width), F32)
    for l in range(leaf_dev):
        x = probes_ref[:, l * width : (l + 1) * width]
        v[l] = x
        v2[l] = stacked(x)
        rr = rr + x * x
    acc[...] = jnp.zeros_like(acc)
    acc2[...] = jnp.zeros_like(acc2)

    pl.semaphore_wait(barrier, n - 1)

    def hop(src, dst, slot, to):
        return pltpu.make_async_remote_copy(
            src_ref=src, dst_ref=dst, send_sem=hsend.at[slot], recv_sem=hrecv.at[slot],
            device_id={"leaf": to}, device_id_type=MESH,
        )

    point_hop = hop(prow.at[pl.ds(0, REACH)], prow.at[pl.ds(leaf_dev, REACH)], 0, before)
    probe_hop = hop(probes_ref.at[:, pl.ds(0, REACH * width)], halo0, 1, before)
    point_hop.start()
    probe_hop.start()

    def products(i, get, into):
        vi = v2[i]
        row = jnp.zeros((width, 2 * cols), F32)
        for o in range(OFFS):
            hi, lo = get(i * OFFS + o, o)
            vj = v2[i + o]
            row = row + dot(hi, vj, 1, 1) + dot(lo, vj, 1, 1)
            if o > 0:
                into[i + o] += fold(dot(vi, hi, 1, 0) + dot(vi, lo, 1, 0))
        into[i] += fold(row.T)

    def build(i, s, o):
        for h in range(0, width, 128):
            listed = mask[pl.ds(s, 1), :]
            right = [
                jnp.broadcast_to(
                    jnp.where(
                        listed > 0.0,
                        prow[i + o, c : c + 1, h : h + 128],
                        prow[i, c : c + 1, h : h + 128],
                    ),
                    (ROWS, 128),
                )
                for c in range(3)
            ]
            top = jnp.broadcast_to(listed, (ROWS, 128))
            for a in range(0, width, ROWS):
                dx = pcb[0, a : a + ROWS, :] - right[0]
                dy = pcb[1, a : a + ROWS, :] - right[1]
                dz = pcb[2, a : a + ROWS, :] - right[2]
                d2 = jnp.maximum(dx * dx + dy * dy + dz * dz, 1e-30)
                u = d2 * lax.rsqrt(d2)
                w = jnp.maximum(top - u, 0.0)
                w = w * w
                w = w * w
                t = w * (d2 + (LIN * u + 1.0 / QUAD)) * jnp.exp2(RATE * u)
                hi, lo = split(t)
                tiles[s, 0, a : a + ROWS, h : h + 128] = hi
                tiles[s, 1, a : a + ROWS, h : h + 128] = lo
        return tiles[s, 0], tiles[s, 1]

    def first_pass(i, carry):
        @pl.when(i == leaf_dev - REACH)
        def _():
            point_hop.wait_recv()
            probe_hop.wait_recv()
            for k in range(REACH):
                x = halo0[:, k * width : (k + 1) * width]
                v[leaf_dev + k] = x
                v2[leaf_dev + k] = stacked(x)

        turned = prow[i].T
        for c in range(3):
            pcb[c] = jnp.broadcast_to(turned[:, c : c + 1], (width, 128))
        products(i, lambda s, o: build(i, s, o), acc)
        return carry

    lax.fori_loop(0, leaf_dev, first_pass, 0)

    lanes = lax.broadcasted_iota(jnp.int32, (cols, 128), 1)

    def share(which, *parts):
        packed = jnp.zeros((cols, 128), F32)
        for k, part in enumerate(parts):
            total = jnp.sum(part, axis=1, keepdims=True)
            packed = jnp.where(lanes == k, total, packed)
        sum_out[which] = packed
        copies = []
        for k in range(1, n):
            slot = which * (n - 1) + k - 1
            copy = pltpu.make_async_remote_copy(
                src_ref=sum_out.at[which], dst_ref=sum_in.at[slot],
                send_sem=ssem.at[slot], recv_sem=rsem.at[slot],
                device_id={"leaf": lax.rem(me + k, n)}, device_id_type=MESH,
            )
            copy.start()
            copies.append(copy)
        return packed, copies

    def collect(which, packed, copies):
        total = packed
        for k, copy in enumerate(copies):
            copy.wait()
            total = total + sum_in[which * (n - 1) + k]
        return total

    back0_hop = hop(acc.at[pl.ds(leaf_dev, REACH)], back0, 2, after)
    back0_hop.start()
    dq = (NUGGET / QUAD) * rr
    for l in range(extent):
        dq = dq + v[l] * acc[l]
    packed, copies = share(0, rr, dq)
    total = collect(0, packed, copies)
    rr0 = total[:, 0:1]
    dq0 = total[:, 1:2] * QUAD
    alpha0 = rr0 / dq0
    back0_hop.wait_recv()

    rr1 = jnp.zeros((cols, width), F32)
    rq = jnp.zeros((cols, width), F32)
    halo_hop = hop(r1.at[pl.ds(0, REACH)], halo1, 3, before)
    for l in range(leaf_dev):
        d = v[l]
        sums = acc[l] + back0[l] if l < REACH else acc[l]
        q = NUGGET * d + QUAD * sums
        r = d - alpha0 * q
        acc[l] = q
        r1[l] = r
        v2[l] = stacked(r)
        rr1 = rr1 + r * r
        rq = rq + r * q
        if l == REACH - 1:
            halo_hop.start()

    def second_pass(i, carry):
        @pl.when(i == leaf_dev - REACH)
        def _():
            halo_hop.wait_recv()
            for k in range(REACH):
                v2[leaf_dev + k] = stacked(halo1[k])

        products(i, lambda s, o: (tiles[s, 0], tiles[s, 1]), acc2)
        return carry

    lax.fori_loop(0, leaf_dev, second_pass, 0)

    back1_hop = hop(acc2.at[pl.ds(leaf_dev, REACH)], back1, 4, after)
    back1_hop.start()
    rw = (NUGGET / QUAD) * rr1
    for l in range(leaf_dev):
        rw = rw + r1[l] * acc2[l]
    for k in range(REACH):
        rw = rw + halo1[k] * acc2[leaf_dev + k]
    packed, copies = share(1, rr1, rw, rq)
    total = collect(1, packed, copies)
    new = total[:, 0:1]
    beta = new / rr0
    curve = total[:, 1:2] * QUAD + beta * (2.0 * total[:, 2:3] + beta * dq0)
    alpha1 = new / curve
    back1_hop.wait_recv()
    for l in range(leaf_dev):
        d = v[l]
        r = r1[l]
        sums = acc2[l] + back1[l] if l < REACH else acc2[l]
        q = NUGGET * r + QUAD * sums + beta * acc[l]
        sol_ref[:, l * width : (l + 1) * width] = alpha0 * d + alpha1 * (r + beta * d)
        res_ref[:, l * width : (l + 1) * width] = r - alpha1 * q
    for copy in (point_hop, probe_hop, back0_hop, halo_hop, back1_hop):
        copy.wait_send()


def body(coords, site_order, leaf_pairs, pair_count, probes):
    n = lax.axis_size("leaf")
    leaf_dev, width = site_order.shape
    cols = probes.shape[0]
    extent = leaf_dev + REACH
    slots = leaf_dev * OFFS
    vmem = pl.BlockSpec(memory_space=pltpu.VMEM)
    smem = pl.BlockSpec(memory_space=pltpu.SMEM)
    field = functools.partial(pltpu.VMEM, dtype=F32)
    return pl.pallas_call(
        functools.partial(kernel, n),
        out_shape=(jax.ShapeDtypeStruct(probes.shape, F32),) * 2,
        in_specs=[vmem, vmem, vmem, smem, vmem],
        out_specs=(vmem, vmem),
        scratch_shapes=[
            field((8, leaf_dev * width)),
            field((extent, 8, width)),
            field((3, width, 128)),
            field((slots, 128)),
            pltpu.VMEM((slots, 2, width, width), BF16),
            field((extent, cols, width)),
            pltpu.VMEM((extent, 2 * cols, width), BF16),
            field((extent, cols, width)),
            field((leaf_dev, cols, width)),
            field((extent, cols, width)),
            field((cols, REACH * width)),
            field((REACH, cols, width)),
            field((REACH, cols, width)),
            field((REACH, cols, width)),
            field((2, cols, 128)),
            field((2 * (n - 1), cols, 128)),
            pltpu.SemaphoreType.DMA((2 * (n - 1),)),
            pltpu.SemaphoreType.DMA((2 * (n - 1),)),
            pltpu.SemaphoreType.DMA((5,)),
            pltpu.SemaphoreType.DMA((5,)),
        ],
        compiler_params=pltpu.CompilerParams(
            collective_id=0, has_side_effects=True, vmem_limit_bytes=56 * 2**20
        ),
    )(coords, site_order, leaf_pairs, pair_count, probes)


def solution(mesh):
    in_specs = (P(None, "leaf"), P("leaf", None), P(None, "leaf"), P("leaf"), P("probe", "leaf"))
    out_specs = (P("probe", "leaf"), P("probe", "leaf"))
    return jax.shard_map(body, mesh=mesh, in_specs=in_specs, out_specs=out_specs, check_vma=False)
```

```python
import functools
import math

import jax
import jax.numpy as jnp
from jax import lax
from jax.experimental import pallas as pl
from jax.experimental.pallas import tpu as pltpu
from jax.sharding import PartitionSpec as P

REACH = 5
UNIT = 0.025
LENGTH = 0.12
NUGGET = 0.5
TAPER = REACH * UNIT
GROW = math.sqrt(3.0) * TAPER / LENGTH
QUAD = 4.0 * GROW
LIN = (4.0 + GROW) / QUAD
RATE = -GROW / math.log(2.0)
OFFS = REACH + 1
ROWS = 32
MESH = pl.DeviceIdType.MESH
F32 = jnp.float32
BF16 = jnp.bfloat16


def split(x):
    hi = x.astype(BF16)
    return hi, (x - hi.astype(F32)).astype(BF16)


def stacked(x):
    hi = x.astype(BF16).astype(F32)
    return jnp.concatenate([hi, x - hi], axis=0).astype(BF16)


def dot(a, b, ca, cb):
    return lax.dot_general(a, b, (((ca,), (cb,)), ((), ())), preferred_element_type=F32)


def fold(x):
    half = x.shape[0] // 2
    return x[:half] + x[half:]


def kernel(
    n, coords_ref, order_ref, pairs_ref, count_ref, probes_ref, sol_ref, res_ref,
    c8, prow, pcb, mask, tiles, v, v2, acc, r1, acc2, twin0, twin1, halo0, halo1,
    part0, part1, back0, back1, sum_out, sum_in, ssem, rsem, hsend, hrecv,
):
    leaf_dev, width = order_ref.shape
    cols = probes_ref.shape[0]
    half = leaf_dev // 2
    span = half + REACH
    me = lax.axis_index("leaf")
    probe = lax.axis_index("probe")
    mine = lax.rem(probe, 2)
    other = 1 - mine
    even = probe - mine
    twin = even + other
    base = half * mine
    twin_base = half * other
    after = lax.rem(me + 1, n)
    before = lax.rem(me + n - 1, n)

    peers = [(k - 1, lax.rem(me + k, n), probe, mine) for k in range(1, n)]
    peers += [(n - 1 + k, lax.rem(me + k, n), twin, other) for k in range(n)]
    slots_in = len(peers)

    barrier = pltpu.get_barrier_semaphore()
    for _, leaf, row, _ in peers:
        pl.semaphore_signal(
            barrier, inc=1, device_id={"leaf": leaf, "probe": row}, device_id_type=MESH
        )

    rr = jnp.zeros((cols, width), F32)
    for l in range(leaf_dev):
        x = probes_ref[:, l * width : (l + 1) * width]
        v[mine, l] = x
        rr = rr + x * x
    v[mine, pl.ds(leaf_dev, REACH)] = jnp.zeros((REACH, cols, width), F32)

    c8[...] = jnp.zeros_like(c8)
    c8[0:3, :] = coords_ref[...] * (1.0 / TAPER)
    place = lax.broadcasted_iota(jnp.int32, (width, width), 0)

    for l in range(leaf_dev):
        x = c8[:, l * width : (l + 1) * width]
        hi = x.astype(BF16).astype(F32)
        mid = (x - hi).astype(BF16).astype(F32)
        parts = jnp.concatenate([hi, mid, x - hi - mid], axis=0).astype(BF16)
        onehot = jnp.where(place == order_ref[l : l + 1, :], 1.0, 0.0).astype(BF16)
        got = dot(parts, onehot, 1, 0)
        prow[l] = got[0:8] + got[8:16] + got[16:24]

    pl.semaphore_wait(barrier, slots_in)

    def hop(src, dst, slot, leaf, row, landing=None):
        return pltpu.make_async_remote_copy(
            src_ref=src, dst_ref=dst, send_sem=hsend.at[slot],
            recv_sem=hrecv.at[slot if landing is None else landing],
            device_id={"leaf": leaf, "probe": row}, device_id_type=MESH,
        )

    twin0_hop = hop(v.at[mine, pl.ds(twin_base, span)], twin0, 0, me, twin)
    point_hop = hop(prow.at[pl.ds(0, REACH)], prow.at[pl.ds(leaf_dev, REACH)], 1, before, probe)
    rim0_hop = hop(v.at[mine, pl.ds(0, REACH)], halo0.at[mine], 2, before, even + 1, 2 + mine)
    rim0_in = [
        hop(v.at[mine, pl.ds(0, REACH)], halo0.at[k], 2, before, even + 1, 2 + k) for k in range(2)
    ]
    twin0_hop.start()
    point_hop.start()
    rim0_hop.start()

    slots = pairs_ref.shape[1]
    first = pairs_ref[0:1, :]
    second = pairs_ref[1:2, :]
    code = (first - me * leaf_dev) * OFFS + (second - first)
    lane = lax.broadcasted_iota(jnp.int32, (1, slots), 1)
    code = jnp.where(lane < count_ref[0], code, -1)
    want = lax.broadcasted_iota(jnp.int32, (leaf_dev * OFFS, slots), 0)
    hit = jnp.max(jnp.where(want == code, 1.0, 0.0), axis=1, keepdims=True)
    mask[...] = jnp.broadcast_to(hit, mask.shape)
    acc[...] = jnp.zeros_like(acc)
    acc2[...] = jnp.zeros_like(acc2)

    def both(field, l):
        return stacked(jnp.concatenate([field[0, l], field[1, l]], axis=0))

    def accept(field, twins):
        for k in range(span):
            field[other, base + k] = twins[k]
        for k in range(span):
            v2[base + k] = both(field, base + k)

    def accept_rim(field, halo):
        for k in range(REACH):
            for r in range(2):
                field[r, leaf_dev + k] = halo[r, k]
            v2[leaf_dev + k] = both(field, leaf_dev + k)

    def add(into, l, x):
        x = fold(x)
        into[0, l] += x[:cols]
        into[1, l] += x[cols:]

    def products(i, get, into):
        vi = v2[i]
        row = jnp.zeros((width, 4 * cols), F32)
        for o in range(OFFS):
            hi, lo = get((i - base) * OFFS + o, o)
            vj = v2[i + o]
            row = row + dot(hi, vj, 1, 1) + dot(lo, vj, 1, 1)
            if o > 0:
                add(into, i + o, dot(vi, hi, 1, 0) + dot(vi, lo, 1, 0))
        add(into, i, row.T)

    def build(i, s, o):
        for h in range(0, width, 128):
            listed = mask[pl.ds(i * OFFS + o, 1), :]
            right = [
                jnp.broadcast_to(
                    jnp.where(
                        listed > 0.0,
                        prow[i + o, c : c + 1, h : h + 128],
                        prow[i, c : c + 1, h : h + 128],
                    ),
                    (ROWS, 128),
                )
                for c in range(3)
            ]
            top = jnp.broadcast_to(listed, (ROWS, 128))
            for a in range(0, width, ROWS):
                dx = pcb[0, a : a + ROWS, :] - right[0]
                dy = pcb[1, a : a + ROWS, :] - right[1]
                dz = pcb[2, a : a + ROWS, :] - right[2]
                d2 = jnp.maximum(dx * dx + dy * dy + dz * dz, 1e-30)
                u = d2 * lax.rsqrt(d2)
                w = jnp.maximum(top - u, 0.0)
                w = w * w
                w = w * w
                t = w * (d2 + (LIN * u + 1.0 / QUAD)) * jnp.exp2(RATE * u)
                hi, lo = split(t)
                tiles[s, 0, a : a + ROWS, h : h + 128] = hi
                tiles[s, 1, a : a + ROWS, h : h + 128] = lo
        return tiles[s, 0], tiles[s, 1]

    twin0_hop.wait_recv()
    accept(v, twin0)

    def first_pass(i, carry):
        @pl.when(i == leaf_dev - REACH)
        def _():
            point_hop.wait_recv()
            for k in range(2):
                rim0_in[k].wait_recv()
            accept_rim(v, halo0)

        turned = prow[i].T
        for c in range(3):
            pcb[c] = jnp.broadcast_to(turned[:, c : c + 1], (width, 128))
        products(i, lambda s, o: build(i, s, o), acc)
        return carry

    lax.fori_loop(base, base + half, first_pass, 0)

    @pl.when(mine == 0)
    def _():
        point_hop.wait_recv()

    lanes = lax.broadcasted_iota(jnp.int32, (cols, 128), 1)

    def overlap(field, sums):
        totals = []
        for r in range(2):
            x = jnp.zeros((cols, width), F32)
            for k in range(span):
                x = x + field[r, base + k] * sums[r, base + k]
            totals.append(jnp.sum(x, axis=1, keepdims=True))
        return totals

    def share(which, shared, own):
        own = [jnp.sum(x, axis=1, keepdims=True) for x in own]
        for r in range(2):
            keep = jnp.where(mine == r, 1.0, 0.0)
            packed = jnp.where(lanes == 0, shared[r], 0.0)
            for k, x in enumerate(own):
                packed = jnp.where(lanes == k + 1, x * keep, packed)
            sum_out[which, r] = packed
        copies = []
        for slot, leaf, row, side in peers:
            at = which * slots_in + slot
            copy = pltpu.make_async_remote_copy(
                src_ref=sum_out.at[which, side], dst_ref=sum_in.at[at],
                send_sem=ssem.at[at], recv_sem=rsem.at[at],
                device_id={"leaf": leaf, "probe": row}, device_id_type=MESH,
            )
            copy.start()
            copies.append(copy)
        return copies

    def collect(which, copies):
        total = sum_out[which, mine]
        for k, copy in enumerate(copies):
            copy.wait()
            total = total + sum_in[which * slots_in + k]
        return total

    def give_back(sums, part, back, slot):
        whole = hop(sums.at[other, pl.ds(base, span)], part, slot, me, twin)
        rims = [
            hop(sums.at[r, pl.ds(leaf_dev, REACH)], back, slot + 1 + r, after, even + r, slot + 1)
            for r in range(2)
        ]
        whole.start()

        @pl.when(mine == 1)
        def _():
            for rim in rims:
                rim.start()

        return whole, rims

    def take_back(sums, part, back, hops):
        whole, rims = hops
        whole.wait_recv()
        for k in range(span):
            sums[mine, twin_base + k] += part[k]
        rims[0].wait_recv()
        for k in range(REACH):
            sums[mine, k] += back[k]
        whole.wait_send()

        @pl.when(mine == 1)
        def _():
            for rim in rims:
                rim.wait_send()

    copies = share(0, overlap(v, acc), [rr])
    hops = give_back(acc, part0, back0, 4)
    total = collect(0, copies)
    rr0 = total[:, 1:2]
    dq0 = total[:, 0:1] * QUAD + NUGGET * rr0
    alpha0 = rr0 / dq0
    take_back(acc, part0, back0, hops)

    rr1 = jnp.zeros((cols, width), F32)
    rq = jnp.zeros((cols, width), F32)
    for l in range(leaf_dev):
        d = v[mine, l]
        q = NUGGET * d + QUAD * acc[mine, l]
        r = d - alpha0 * q
        acc[mine, l] = q
        r1[mine, l] = r
        rr1 = rr1 + r * r
        rq = rq + r * q
    r1[mine, pl.ds(leaf_dev, REACH)] = jnp.zeros((REACH, cols, width), F32)
    twin1_hop = hop(r1.at[mine, pl.ds(twin_base, span)], twin1, 7, me, twin)
    rim1_hop = hop(r1.at[mine, pl.ds(0, REACH)], halo1.at[mine], 8, before, even + 1, 8 + mine)
    rim1_in = [
        hop(r1.at[mine, pl.ds(0, REACH)], halo1.at[k], 8, before, even + 1, 8 + k) for k in range(2)
    ]
    twin1_hop.start()
    rim1_hop.start()
    twin1_hop.wait()
    accept(r1, twin1)

    def second_pass(i, carry):
        @pl.when(i == leaf_dev - REACH)
        def _():
            for k in range(2):
                rim1_in[k].wait_recv()
            accept_rim(r1, halo1)

        products(i, lambda s, o: (tiles[s, 0], tiles[s, 1]), acc2)
        return carry

    lax.fori_loop(base, base + half, second_pass, 0)

    copies = share(1, overlap(r1, acc2), [rr1, rq])
    hops = give_back(acc2, part1, back1, 10)
    total = collect(1, copies)
    new = total[:, 1:2]
    beta = new / rr0
    curve = total[:, 0:1] * QUAD + NUGGET * new + beta * (2.0 * total[:, 2:3] + beta * dq0)
    alpha1 = new / curve
    take_back(acc2, part1, back1, hops)
    for l in range(leaf_dev):
        d = v[mine, l]
        r = r1[mine, l]
        q = NUGGET * r + QUAD * acc2[mine, l] + beta * acc[mine, l]
        sol_ref[:, l * width : (l + 1) * width] = alpha0 * d + alpha1 * (r + beta * d)
        res_ref[:, l * width : (l + 1) * width] = r - alpha1 * q
    for copy in (twin0_hop, point_hop, rim0_hop, rim1_hop):
        copy.wait_send()


def body(coords, site_order, leaf_pairs, pair_count, probes):
    n = lax.axis_size("leaf")
    leaf_dev, width = site_order.shape
    cols = probes.shape[0]
    extent = leaf_dev + REACH
    span = leaf_dev // 2 + REACH
    slots_in = 2 * n - 1
    vmem = pl.BlockSpec(memory_space=pltpu.VMEM)
    smem = pl.BlockSpec(memory_space=pltpu.SMEM)
    field = functools.partial(pltpu.VMEM, dtype=F32)
    return pl.pallas_call(
        functools.partial(kernel, n),
        out_shape=(jax.ShapeDtypeStruct(probes.shape, F32),) * 2,
        in_specs=[vmem, vmem, vmem, smem, vmem],
        out_specs=(vmem, vmem),
        scratch_shapes=[
            field((8, leaf_dev * width)),
            field((extent, 8, width)),
            field((3, width, 128)),
            field((leaf_dev * OFFS, 128)),
            pltpu.VMEM((leaf_dev // 2 * OFFS, 2, width, width), BF16),
            field((2, extent, cols, width)),
            pltpu.VMEM((extent, 4 * cols, width), BF16),
            field((2, extent, cols, width)),
            field((2, extent, cols, width)),
            field((2, extent, cols, width)),
            field((span, cols, width)),
            field((span, cols, width)),
            field((2, REACH, cols, width)),
            field((2, REACH, cols, width)),
            field((span, cols, width)),
            field((span, cols, width)),
            field((REACH, cols, width)),
            field((REACH, cols, width)),
            field((2, 2, cols, 128)),
            field((2 * slots_in, cols, 128)),
            pltpu.SemaphoreType.DMA((2 * slots_in,)),
            pltpu.SemaphoreType.DMA((2 * slots_in,)),
            pltpu.SemaphoreType.DMA((13,)),
            pltpu.SemaphoreType.DMA((13,)),
        ],
        compiler_params=pltpu.CompilerParams(
            collective_id=0, has_side_effects=True, vmem_limit_bytes=48 * 2**20
        ),
    )(coords, site_order, leaf_pairs, pair_count, probes)


def solution(mesh):
    in_specs = (P(None, "leaf"), P("leaf", None), P(None, "leaf"), P("leaf"), P("probe", "leaf"))
    out_specs = (P("probe", "leaf"), P("probe", "leaf"))
    return jax.shard_map(body, mesh=mesh, in_specs=in_specs, out_specs=out_specs, check_vma=False)
```
